32 devices in a mesh: grp: 4 (over x, core), dev: 8 (over z, y).
Axes of the slice: x: 2, y: 2, z: 4, core: 2. Of those that a mesh axis runs over, the one named last changes fastest.
Arguments:
- density: bfloat16 [12288, 12288], P('grp', 'dev'), may hold values from -0.0546875 to 0.0546875
- left_factor: bfloat16 [512, 12288], P('dev', 'grp'), may hold values from -3 to 3
- right_factor: bfloat16 [512, 12288], P(None, 'dev'), may hold values from -3 to 3
- directions: float32 [3, 12288], P(None, 'dev'), may hold values from -1 to 1
- places: float32 [3, 4, 8, 4096], P(None, 'grp', 'dev'), may hold values from 0 to 8, as said below
- alpha: float32 [4, 8, 4096], P('grp', 'dev'), may hold values from 0.4 to 1.6
- static_field: float32 [3, 4, 8, 4096], P(None, 'grp', 'dev'), may hold values from -6 to 6
- neighbours: int32 [4, 8, 32, 12], P('grp', 'dev'), may hold values from 0 to 287, as said below
- targets: int32 [4, 8, 16], P('grp', 'dev'), may hold values from 0 to 4095, as said below
Outputs:
- dipoles: float32 [3, 4, 8, 4096], P(None, 'grp', 'dev')
- qm_field: float32 [3, 512], P(None, ('grp', 'dev'))
- fock_polar: float32 [12288, 12288], P('grp', 'dev')
The draws below stay inside these ranges and needn't reach their ends.
Inputs may be any that keep to these rules, and one draw needn't show every extreme that they name: `places`: site s of brick (g, d) lies at x in [0.1 g, 0.1 (g + 1)), y in [0.1 d, 0.1 (d + 1)), z in [0.03 k, 0.03 (k + 1)) with k = s // 128. `neighbours`: entries of one row differ; the first names the block itself (brick part 4, the centre of the 3 x 3 bricks, i.e. 4 * 32 + b); every entry names a block of the 3 x 3 bricks around the own brick whose index along the third coordinate is within 2 of the block's own and inside 0 to 31. The targets of one brick are distinct sites.
All inputs are finite; a program needn't handle non-finite values.
Results may differ from the reference program's by a relative error of at most 0.0029.
Values may be sent and summed in bfloat16 or wider, within the bound.
No kernel may reach another device: no remote copies, remote signals or barrier semaphores. Data moves between devices by JAX's collectives and lax.ppermute only.
A program may use at most 128 MiB of HBM per device.

```python
import math
import jax
import jax.numpy as jnp
from jax import lax

NB = 12288
BS = 128
NNB = 12
SWEEPS = 4
SB = 4096
TPD = 16
NG = 4
ND = 8
NBLK = 32
NT = 512


def draw_places(key, part):
    uniform_draw = jax.random.uniform(jax.random.fold_in(key, 11), (3, NG, ND, SB), jnp.float32)
    row_brick = jnp.arange(NG).astype(jnp.float32)[:, None, None]
    col_brick = jnp.arange(ND).astype(jnp.float32)[None, :, None]
    slab = (jnp.arange(SB) // BS).astype(jnp.float32)[None, None, :]
    depth = uniform_draw[2]
    first = (row_brick + uniform_draw[0]) * 0.1
    second = (col_brick + uniform_draw[1]) * 0.1
    third = (slab + depth) * 0.03
    return jnp.stack([first, second, third]).astype(jnp.float32)


def draw_neighbours(key, part):
    count = NG * ND * NBLK
    keys = jax.random.split(jax.random.fold_in(key, 23), count)
    scores = jax.vmap(lambda single: jax.random.permutation(single, 27))(keys).astype(jnp.int32)
    block = jnp.arange(count, dtype=jnp.int32) % NBLK
    lowest = jnp.clip(block - 1, 0, NBLK - 3)
    itself = 12 + (block - lowest)
    candidate = jnp.arange(27, dtype=jnp.int32)
    scores = jnp.where(candidate[None, :] == itself[:, None], -1, scores)
    order = jnp.argsort(scores, axis=1)[:, :NNB].astype(jnp.int32)
    slot = order // 3
    chosen = lowest[:, None] + order % 3
    links = slot * NBLK + chosen
    return links.reshape(NG, ND, NBLK, NNB).astype(jnp.int32)


def draw_targets(key, part):
    keys = jax.random.split(jax.random.fold_in(key, 37), NG * ND)
    picked = jax.vmap(lambda single: jax.random.permutation(single, SB)[:TPD])(keys)
    return picked.reshape(NG, ND, TPD).astype(jnp.int32)


def block_scale(key, shape, cuts, smallest, high):
    def one(dim, blocks):
        draws = jax.random.uniform(jax.random.fold_in(jax.random.fold_in(key, 6), dim), (blocks,), jnp.float32, smallest / len(cuts), high / len(cuts))
        return jnp.repeat(jnp.exp(draws), shape[dim] // blocks).reshape((-1,) + (1,) * (len(shape) - dim - 1))

    gain = one(*cuts[0])
    for cut in cuts[1:]:
        gain = gain * one(*cut)
    return gain


def gaussian(key, dims, spread, reach, cuts=(), kind=jnp.bfloat16):
    array = spread * jax.random.normal(key, dims, jnp.float32)
    if cuts:
        array = array * block_scale(key, dims, cuts, -0.22, 0.18)
    return jnp.clip(array, -reach, reach).astype(kind)


def setup_inputs(seed: int = 0) -> dict:
    arg_keys = jax.random.split(jax.random.key(seed), 10)
    return {
        "density": gaussian(arg_keys[0], (NB, NB), (2.0 * NT ** 0.5 / NB), 0.0546875, ((0, 4), (1, 8))),
        "left_factor": gaussian(arg_keys[1], (NT, NB), (NT ** -0.25), 3.0, ((0, 8), (1, 4))),
        "right_factor": gaussian(arg_keys[2], (NT, NB), (NT ** -0.25), 3.0, ((1, 8),)),
        "directions": jnp.clip(jax.random.uniform(arg_keys[3], (3, NB), jnp.float32, -1.0, 1.0) * block_scale(arg_keys[3], (3, NB), ((1, 8),), -0.4, 0.0), -1.0, 1.0),
        "places": draw_places(jax.random.fold_in(arg_keys[9], 71), 0),
        "alpha": jnp.clip(jnp.exp(math.log(1.6) - 1.3862944 * jax.random.uniform(arg_keys[5], (NG, ND, SB), jnp.float32) ** block_scale(arg_keys[5], (NG, ND, SB), ((0, 4), (1, 8)), -0.2, 0.2)), 0.4, 1.6),
        "static_field": gaussian(arg_keys[6], (3, NG, ND, SB), 1.0, 6.0, ((1, 4), (2, 8)), jnp.float32),
        "neighbours": draw_neighbours(jax.random.fold_in(arg_keys[9], 71), 0),
        "targets": draw_targets(jax.random.fold_in(arg_keys[9], 71), 0),
    }


coupling = 2e-07
soften = 4e-05
blocks_per_turn = 4

def pair_field(own_sites, region_places, region_dipoles, links):
    blocks, listed = links.shape
    width = region_places.shape[2]
    turns = blocks // blocks_per_turn
    own_groups = own_sites.reshape(3, turns, blocks_per_turn, width).transpose(1, 0, 2, 3)
    link_groups = links.reshape(turns, blocks_per_turn, listed)
    column = jnp.arange(listed * width, dtype=jnp.int32)[None, :]
    row_ids = jnp.arange(width, dtype=jnp.int32)[:, None]
    keeper = column != row_ids

    def one_group(pieces):
        own_group, link_group = pieces
        near_places = region_places[:, link_group].reshape(3, blocks_per_turn, listed * width)
        near_dipoles = region_dipoles[:, link_group].reshape(3, blocks_per_turn, listed * width)
        offsets = own_group[:, :, :, None] - near_places[:, :, None, :]
        square = lax.optimization_barrier(jnp.sum(offsets * offsets, axis=0)) + soften
        inverse_cube = jnp.where(keeper, lax.rsqrt(square) / square, jnp.zeros_like(square))
        inverse_fifth = inverse_cube / square
        projection = lax.optimization_barrier(jnp.sum(offsets * near_dipoles[:, :, None, :], axis=0))
        first_part = 3.0 * lax.optimization_barrier(jnp.sum(offsets * (projection * inverse_fifth)[None], axis=-1))
        second_part = lax.optimization_barrier(jnp.sum(near_dipoles[:, :, None, :] * inverse_cube[None], axis=-1))
        return coupling * (first_part - second_part)
    fields = lax.map(one_group, (own_groups, link_groups))
    return fields.transpose(1, 0, 2, 3).reshape(3, blocks * width)

def reference(density, left_factor, right_factor, directions, places, alpha, static_field, neighbours, targets):
    context = jnp.dot(left_factor, density, preferred_element_type=jnp.float32)
    weighted = context * right_factor.astype(jnp.float32)
    qm_field = jnp.einsum('tn,kn->kt', weighted, directions, precision=lax.Precision.HIGHEST)
    picks = (targets[:, :, :, None] == jnp.arange(SB, dtype=jnp.int32)[None, None, None, :]).astype(jnp.float32)
    total = static_field + jnp.einsum('kgdt,gdts->kgds', qm_field.reshape(3, NG, ND, TPD), picks, precision=lax.Precision.HIGHEST)
    dipoles = alpha[None] * total
    padded_places = jnp.pad(places, ((0, 0), (1, 1), (1, 1), (0, 0)))
    zero = jnp.int32(0)

    def brick_field(brick, padded_dipoles):
        row_brick = (brick // ND).astype(jnp.int32)
        col_brick = (brick % ND).astype(jnp.int32)
        region_places = lax.dynamic_slice(padded_places, (zero, row_brick, col_brick, zero), (3, 3, 3, SB)).reshape(3, 9 * NBLK, BS)
        region_dipoles = lax.dynamic_slice(padded_dipoles, (zero, row_brick, col_brick, zero), (3, 3, 3, SB)).reshape(3, 9 * NBLK, BS)
        own_sites = lax.dynamic_slice(places, (zero, row_brick, col_brick, zero), (3, 1, 1, SB)).reshape(3, SB)
        links = lax.dynamic_slice(neighbours, (row_brick, col_brick, zero, zero), (1, 1, NBLK, NNB)).reshape(NBLK, NNB)
        return pair_field(own_sites, region_places, region_dipoles, links)
    for repeat in range(SWEEPS):
        padded_dipoles = jnp.pad(dipoles, ((0, 0), (1, 1), (1, 1), (0, 0)))
        fields = lax.map(lambda brick: brick_field(brick, padded_dipoles), jnp.arange(NG * ND, dtype=jnp.int32))
        fields = fields.reshape(NG, ND, 3, SB).transpose(2, 0, 1, 3)
        dipoles = alpha[None] * (total + fields)
    target_dipoles = jnp.einsum('kgds,gdts->kgdt', dipoles, picks, precision=lax.Precision.HIGHEST).reshape(3, NT)
    along = jnp.einsum('kt,kn->tn', target_dipoles, directions, precision=lax.Precision.HIGHEST)
    scaled = (right_factor.astype(jnp.float32) * along).astype(jnp.bfloat16)
    fock_polar = -jnp.dot(left_factor.T, scaled, preferred_element_type=jnp.float32)
    return (dipoles, qm_field, fock_polar)
```

```python
import functools

import jax
import jax.numpy as jnp
from jax import lax
from jax.experimental import pallas as pl
from jax.experimental.pallas import tpu as pltpu
from jax.sharding import PartitionSpec as P

SWEEPS = 4
COUPLING = 2e-07
SOFTEN = 4e-05
BRICK = 0.1
SLAB = 0.03
REACH = 2
BOTH = ("grp", "dev")
F32 = jnp.float32
BF16 = jnp.bfloat16
FEATS = 32
TERMS = 16
PARTS = 3
VMEM = pl.BlockSpec(memory_space=pltpu.VMEM)
SMEM = pl.BlockSpec(memory_space=pltpu.SMEM)


def shift(block, axis, step):
    count = lax.axis_size(axis)
    pairs = [(i, i + step) for i in range(count) if 0 <= i + step < count]
    return lax.ppermute(block, axis, pairs)


def exchange(block):
    column = jnp.stack([shift(block, "grp", 1), block, shift(block, "grp", -1)])
    return shift(column, "dev", 1), column, shift(column, "dev", -1)


def rounded(value):
    return value.astype(BF16).astype(F32)


def features(coords, own):
    x, y, z = coords
    width = x.shape[1]
    row = lax.broadcasted_iota(jnp.int32, (FEATS, width), 0)
    norm = x * x + y * y + z * z
    if own:
        norm = norm + SOFTEN
    first = 21 if own else 18
    is_norm = (row >= first) & (row < first + 3)
    is_one = (row >= 18) & (row < 24) & ~is_norm
    value = jnp.where(row < 6, x, jnp.where(row < 12, y, jnp.where(row < 18, z, norm)))
    high = rounded(value)
    rest = value - high
    middle = rounded(rest)
    low = rest - middle
    kind = lax.rem(row, 6)
    if own:
        kinds = (0, 0, 1, 0, 2, 1)
    else:
        kinds = (0, 1, 0, 2, 0, 1)
    level = jnp.zeros_like(row)
    for at, which in enumerate(kinds):
        level = jnp.where((row < 18) & (kind == at), which, level)
    level = jnp.where(is_norm, row - first, level)
    part = jnp.where(level == 0, high, jnp.where(level == 1, middle, low))
    if own:
        part = jnp.where(row < 18, -2.0 * part, part)
    part = jnp.where(is_one, 1.0, part)
    part = jnp.where(row < 24, part, 0.0)
    return part.astype(BF16)


def weights_kernel(per_step, blocks, links_ref, coords_ref, out_ref, far_ref, own_ref):
    step = pl.program_id(0)
    region = coords_ref.shape[1]
    width = coords_ref.shape[2]
    listed = out_ref.shape[1] // width
    own_base = region // 9 * 4

    def row_of(at):
        return tuple(coords_ref[k, pl.ds(at, 1), :] for k in range(3))

    @pl.when(step == 0)
    def _():
        def fill(at, carry):
            far_ref[at] = features(row_of(at), False)
            return carry

        lax.fori_loop(0, region, fill, 0, unroll=4)

    diagonal = lax.broadcasted_iota(jnp.int32, (width, width), 0) == lax.broadcasted_iota(
        jnp.int32, (width, width), 1
    )
    for inner in range(per_step):
        block = step * per_step + inner
        x, y, z = row_of(own_base + block)
        for at in range(2 * REACH + 1):
            own_ref[inner, at] = features((x, y, z - (at - REACH) * SLAB), True)
    for inner in range(per_step):
        block = step * per_step + inner
        for n in range(listed):
            link = links_ref[block, n]
            hop = lax.rem(link, blocks) - block + REACH
            square = lax.dot_general(
                far_ref[link],
                own_ref[inner, hop],
                (((0,), (0,)), ((), ())),
                preferred_element_type=F32,
            )
            root = lax.rsqrt(square)
            two = root * root
            value = two * two * root
            if n == 0:
                value = jnp.where(diagonal, 0.0, value)
            out_ref[inner, n * width : (n + 1) * width, :] = value.astype(BF16)


def pair_weights(links, coords, blocks):
    listed = links.shape[1]
    region, width = coords.shape[1:]
    per_step = 2
    return pl.pallas_call(
        functools.partial(weights_kernel, per_step, blocks),
        out_shape=jax.ShapeDtypeStruct((blocks, listed * width, width), BF16),
        grid=(blocks // per_step,),
        in_specs=[SMEM, pl.BlockSpec((3, region, width), lambda i: (0, 0, 0))],
        out_specs=pl.BlockSpec((per_step, listed * width, width), lambda i: (i, 0, 0)),
        scratch_shapes=[
            pltpu.VMEM((region, FEATS, width), BF16),
            pltpu.VMEM((per_step, 2 * REACH + 1, FEATS, width), BF16),
        ],
        name="pair_weights",
    )(links, coords)


def sweep_kernel(
    per_step,
    blocks,
    first,
    last,
    base,
    at_ref,
    links_ref,
    target_ref,
    polar_ref,
    field_ref,
    coords_ref,
    low_ref,
    mid_ref,
    high_ref,
    weights_ref,
    alpha_ref,
    total_ref,
    *rest,
):
    if first:
        out_ref, sum_ref, v_ref, w_ref, p_ref = rest
    elif last:
        out_ref, pick_ref, v_ref, w_ref, p_ref = rest
    else:
        out_ref, v_ref, w_ref, p_ref = rest
    step = pl.program_id(0)
    region, width = coords_ref.shape[1:]
    listed = weights_ref.shape[1] // width
    own_base = 4 * blocks
    lane = lax.broadcasted_iota(jnp.int32, (1, width), 1)

    @pl.when(step == 0)
    def _():
        for a in range(3):
            for b, ref in enumerate((low_ref, mid_ref, high_ref)):
                for k in range(3):
                    v_ref[k, (3 * a + b) * blocks : (3 * a + b + 1) * blocks, :] = ref[
                        a, base + k * blocks : base + (k + 1) * blocks, :
                    ]
        if first:
            per_brick = target_ref.shape[1]
            groups, members = at_ref[2], at_ref[3]
            per_row = field_ref.shape[1] // per_brick
            sum_ref[...] = total_ref[...]

            def brick(p, carry):
                grp = jnp.clip(at_ref[0] + p // 3 - 1, 0, groups - 1)
                dev = jnp.clip(at_ref[1] + p % 3 - 1, 0, members - 1)
                owner = grp * members + dev
                chunk = owner // per_row
                start = owner % per_row * per_brick

                def one(j, inner):
                    site = target_ref[p, j]
                    here = lane == site % width
                    row = p * blocks + site // width
                    for k in range(3):
                        value = field_ref[chunk * 3 + k, start + j]
                        add = jnp.where(here, value * polar_ref[p, j], 0.0)
                        v_ref[k, pl.ds(row, 1), :] += add
                    return inner

                return lax.fori_loop(0, per_brick, one, carry, unroll=4)

            lax.fori_loop(0, 9, brick, 0)
            owner = at_ref[0] * members + at_ref[1]
            chunk = owner // per_row
            start = owner % per_row * per_brick

            def mine(j, carry):
                site = target_ref[4, j]
                here = lane == site % width
                for k in range(3):
                    value = field_ref[chunk * 3 + k, start + j]
                    sum_ref[pl.ds(k * blocks + site // width, 1), :] += jnp.where(here, value, 0.0)
                return carry

            lax.fori_loop(0, per_brick, mine, 0, unroll=4)

    row = lax.broadcasted_iota(jnp.int32, (TERMS, width), 0)
    which = lax.rem(row, 3)
    for inner in range(per_step):
        block = step * per_step + inner
        for n in range(listed):
            link = links_ref[block, n]
            away = (lax.rem(link, blocks) - block).astype(F32) * SLAB
            x = coords_ref[0, pl.ds(link, 1), :]
            y = coords_ref[1, pl.ds(link, 1), :]
            z = coords_ref[2, pl.ds(link, 1), :] + away
            v0, v1, v2 = (v_ref[k, pl.ds(link, 1), :] for k in range(3))
            along = x * v0 + y * v1 + z * v2
            third = (x * x + y * y + z * z) * (1.0 / 3.0)
            dipole = jnp.where(which == 0, v0, jnp.where(which == 1, v1, v2))
            place = jnp.where(
                row < 3,
                1.0,
                jnp.where(
                    (row < 6) | (row == 12), x, jnp.where((row < 9) | (row == 13), y, z)
                ),
            )
            value = jnp.where(row < 12, place * dipole, place * along - third * dipole)
            cols = slice(n * width, (n + 1) * width)
            for part in range(PARTS):
                piece = value.astype(BF16)
                w_ref[inner, part * TERMS : (part + 1) * TERMS, cols] = piece
                if part < PARTS - 1:
                    value = value - piece.astype(F32)
        product = jnp.dot(w_ref[inner], weights_ref[inner], preferred_element_type=F32)
        total = product[:TERMS]
        for part in range(1, PARTS):
            total = total + product[part * TERMS : (part + 1) * TERMS]
        p_ref[block] = total

    @pl.when(step == pl.num_programs(0) - 1)
    def _():
        x = [coords_ref[k, own_base : own_base + blocks, :] for k in range(3)]
        term = [p_ref[:, r, :] for r in range(15)]
        p = term[:3]
        m = [term[3 + 3 * k : 6 + 3 * k] for k in range(3)]
        q = term[12:15]
        inside = x[0] * p[0] + x[1] * p[1] + x[2] * p[2] - (m[0][0] + m[1][1] + m[2][2])
        size = x[0] * x[0] + x[1] * x[1] + x[2] * x[2] + SOFTEN
        alpha = alpha_ref[...]
        for k in range(3):
            one = x[0] * m[k][0] + x[1] * m[k][1] + x[2] * m[k][2]
            other = x[0] * m[0][k] + x[1] * m[1][k] + x[2] * m[2][k]
            force = x[k] * inside - one + q[k] - (size * p[k] - 2.0 * other) * (1.0 / 3.0)
            rows = slice(k * blocks, (k + 1) * blocks)
            given = sum_ref[rows, :] if first else total_ref[rows, :]
            out_ref[rows, :] = alpha * (given + (3.0 * COUPLING) * force)
        if last:
            per_brick = target_ref.shape[1]
            pick_ref[...] = jnp.zeros_like(pick_ref)

            def pick(j, carry):
                site = target_ref[4, j]
                here = lane == site % width
                line = jnp.zeros((1, width), F32)
                for k in range(3):
                    values = out_ref[pl.ds(k * blocks + site // width, 1), :]
                    found = jnp.sum(jnp.where(here, values, 0.0), axis=1, keepdims=True)
                    line = jnp.where(lane == k, found, line)
                pick_ref[pl.ds(j, 1), :] = line
                return carry

            lax.fori_loop(0, per_brick, pick, 0, unroll=True)


def sweep(at, links, targets, polar, field, coords, around, weights, alpha, total, first, last, base):
    blocks, depth, width = weights.shape
    region = coords.shape[1]
    per_step = 4
    outs = [jax.ShapeDtypeStruct((3 * blocks, width), F32)]
    if first:
        outs.append(jax.ShapeDtypeStruct((3 * blocks, width), F32))
    if last:
        outs.append(jax.ShapeDtypeStruct((targets.shape[1], width), F32))

    def whole(array):
        return pl.BlockSpec(array.shape, lambda i: (0,) * len(array.shape))

    return pl.pallas_call(
        functools.partial(sweep_kernel, per_step, blocks, first, last, base),
        out_shape=outs,
        grid=(blocks // per_step,),
        in_specs=[
            SMEM,
            SMEM,
            SMEM,
            SMEM,
            SMEM,
            whole(coords),
            whole(around[0]),
            whole(around[1]),
            whole(around[2]),
            pl.BlockSpec((per_step, depth, width), lambda i: (i, 0, 0)),
            whole(alpha),
            whole(total),
        ],
        out_specs=[whole(o) for o in outs],
        scratch_shapes=[
            pltpu.VMEM((3, region, width), F32),
            pltpu.VMEM((per_step, PARTS * TERMS, depth), BF16),
            pltpu.VMEM((blocks, TERMS, width), F32),
        ],
        name="sweep",
    )(at, links, targets, polar, field, coords, *around, weights, alpha, total)


def context_kernel(count, source_ref, *refs):
    lefts = refs[:count]
    density_ref = refs[count]
    rights = refs[count + 1 : 2 * count + 1]
    directions_ref, out_ref, left_ref, sums_ref = refs[2 * count + 1 :]
    step = pl.program_id(0)
    rows = lefts[0].shape[0]

    @pl.when(step == 0)
    def _():
        for i, ref in enumerate(lefts):
            left_ref[i * rows : (i + 1) * rows, :] = ref[...]
        sums_ref[...] = jnp.zeros_like(sums_ref)

    context = jnp.dot(left_ref[...], density_ref[...], preferred_element_type=F32)
    lanes = context.shape[1]
    for i, ref in enumerate(rights):
        weighted = context[i * rows : (i + 1) * rows] * ref[...].astype(F32)
        for k in range(3):
            term = weighted * directions_ref[k : k + 1, :]
            folded = term[:, :128]
            for at in range(128, lanes, 128):
                folded = folded + term[:, at : at + 128]
            sums_ref[k, i * rows : (i + 1) * rows, :] += folded

    @pl.when(step == pl.num_programs(0) - 1)
    def _():
        for k in range(3):
            for at in range(0, sums_ref.shape[1], 128):
                flipped = jnp.transpose(sums_ref[k, at : at + 128, :])
                out_ref[k : k + 1, at : at + 128] = jnp.sum(flipped, axis=0, keepdims=True)


def context_field(sources, chunks, density, right, directions):
    count = len(chunks)
    rows, depth = chunks[0].shape
    columns = density.shape[1]
    tile = 256
    padded = -(-count * rows // 128) * 128

    def right_block(i):
        return pl.BlockSpec((rows, tile), lambda j, source: (source[i], j))

    return pl.pallas_call(
        functools.partial(context_kernel, count),
        out_shape=jax.ShapeDtypeStruct((3, padded), F32),
        grid_spec=pltpu.PrefetchScalarGridSpec(
            num_scalar_prefetch=1,
            grid=(columns // tile,),
            in_specs=[pl.BlockSpec((rows, depth), lambda j, source: (0, 0)) for _ in chunks]
            + [pl.BlockSpec((depth, tile), lambda j, source: (0, j))]
            + [right_block(i) for i in range(count)]
            + [pl.BlockSpec((3, tile), lambda j, source: (0, j))],
            out_specs=pl.BlockSpec((3, padded), lambda j, source: (0, 0)),
            scratch_shapes=[
                pltpu.VMEM((count * rows, depth), BF16),
                pltpu.VMEM((3, padded, 128), F32),
            ],
        ),
        name="context_field",
    )(sources, *chunks, density, *([right] * count), directions)


def fock_kernel(count, source_ref, *refs):
    lefts = refs[:count]
    right_ref, directions_ref, dipoles_ref, out_ref, scaled_ref = refs[count:]
    rows = lefts[0].shape[0]

    @pl.when(pl.program_id(0) == 0)
    def _():
        lines = [directions_ref[k : k + 1, :] for k in range(3)]
        for i in range(count):
            start = pl.multiple_of(source_ref[i] * rows, rows)
            dipoles = dipoles_ref[pl.ds(start, rows), :]
            along = dipoles[:, 0:1] * lines[0]
            for k in (1, 2):
                along = along + dipoles[:, k : k + 1] * lines[k]
            value = right_ref[pl.ds(start, rows), :].astype(F32) * along
            scaled_ref[i * rows : (i + 1) * rows, :] = (-value).astype(BF16)

    left = jnp.concatenate([ref[...] for ref in lefts], axis=0)
    out_ref[...] = lax.dot_general(
        left, scaled_ref[...], (((0,), (0,)), ((), ())), preferred_element_type=F32
    )


def fock_term(sources, chunks, right, directions, dipoles):
    count = len(chunks)
    rows, depth = chunks[0].shape
    targets, columns = right.shape
    tile = 512

    def whole(array):
        return pl.BlockSpec(array.shape, lambda i, source: (0,) * len(array.shape))

    return pl.pallas_call(
        functools.partial(fock_kernel, count),
        out_shape=jax.ShapeDtypeStruct((depth, columns), F32),
        grid_spec=pltpu.PrefetchScalarGridSpec(
            num_scalar_prefetch=1,
            grid=(depth // tile,),
            in_specs=[pl.BlockSpec((rows, tile), lambda i, source: (0, i)) for _ in chunks]
            + [whole(right), whole(directions), whole(dipoles)],
            out_specs=pl.BlockSpec((tile, columns), lambda i, source: (i, 0)),
            scratch_shapes=[pltpu.VMEM((targets, columns), BF16)],
        ),
        name="fock_term",
    )(sources, *chunks, right, directions, dipoles)


def ring_order(count):
    return list(range(0, count, 2)) + [i for i in range(count - 1, 0, -1) if i % 2]


def on_device(
    density, left_factor, right_factor, directions, places, alpha, static_field, neighbours, targets
):
    groups = lax.axis_size("grp")
    members = lax.axis_size("dev")
    grp = lax.axis_index("grp")
    dev = lax.axis_index("dev")
    rows = left_factor.shape[0]
    per_brick = targets.shape[2]
    sites = places.shape[3]
    blocks = neighbours.shape[2]
    width = sites // blocks
    devices = groups * members

    links = neighbours[0, 0]
    polar = alpha[0, 0]
    own_targets = targets[0, 0]
    fixed = static_field[:, 0, 0]
    picked = jnp.sum(
        jnp.where(own_targets[:, None] == jnp.arange(sites, dtype=jnp.int32)[None, :], polar[None, :], 0.0),
        axis=1,
    )
    tail = jnp.zeros((8, width), F32)
    tail = tail.at[0, :per_brick].set(own_targets.astype(F32)).at[1, :per_brick].set(picked)
    packed = jnp.concatenate(
        [
            places[:, 0, 0].reshape(3 * blocks, width),
            (polar[None] * fixed).reshape(3 * blocks, width),
            tail,
        ]
    )
    around = exchange(packed)
    everything = jnp.stack(around, axis=1).reshape(9, packed.shape[0], width)
    region = everything[:, : 3 * blocks].reshape(9, 3, blocks, width).transpose(1, 0, 2, 3)
    region = region.reshape(3, 9 * blocks, width)
    level = (jnp.arange(9 * blocks, dtype=jnp.int32) % blocks).astype(F32)
    middle_x = (grp.astype(F32) + 0.5) * BRICK
    middle_y = (dev.astype(F32) + 0.5) * BRICK
    middle_z = (level + 0.5) * SLAB
    coords = jnp.stack([region[0] - middle_x, region[1] - middle_y, region[2] - middle_z[:, None]])
    nearby_targets = everything[:, 6 * blocks, :per_brick].astype(jnp.int32)
    nearby_polar = everything[:, 6 * blocks + 1, :per_brick]
    weights = pair_weights(links, coords, blocks)

    order = ring_order(members)
    place_of = [order.index(i) for i in range(members)]
    order_table = jnp.array(order, jnp.int32)
    position = jnp.array(place_of, jnp.int32)[dev]
    forward = [(order[i], order[(i + 1) % members]) for i in range(members)]
    backward = [(b, a) for a, b in forward]
    chunks = {0: left_factor}
    onward = back = left_factor
    groups_of = [[0]]
    for step in range(1, members // 2 + 1):
        onward = lax.ppermute(onward, "dev", forward)
        chunks[-step] = onward
        fresh = [-step]
        if step <= (members - 1) // 2:
            back = lax.ppermute(back, "dev", backward)
            chunks[step] = back
            fresh.append(step)
        groups_of.append(fresh)
    if len(groups_of) > 1:
        groups_of = [groups_of[0] + groups_of[1]] + groups_of[2:]
    if len(groups_of) > 2 and len(groups_of[-1]) == 1:
        groups_of = groups_of[:-2] + [groups_of[-2] + groups_of[-1]]

    def source_of(offset):
        return order_table[lax.rem(position + offset + members, members)]

    fields = {}
    for offsets in groups_of:
        sources = jnp.stack([source_of(o) for o in offsets])
        part = context_field(sources, [chunks[o] for o in offsets], density, right_factor, directions)
        for i, offset in enumerate(offsets):
            fields[offset % members] = part[:, i * rows : (i + 1) * rows]
    by_offset = jnp.stack([fields[o] for o in range(members)])
    back_offset = lax.rem(jnp.array(place_of, jnp.int32) - position + members, members)
    partial = jnp.take(by_offset, back_offset, axis=0).reshape(members * 3, rows)
    spread = jnp.broadcast_to(partial[None], (devices,) + partial.shape)
    field = jnp.sum(lax.all_to_all(spread, BOTH, 0, 0), axis=0)
    owner = grp * members + dev
    local = lax.dynamic_slice_in_dim(field.reshape(members, 3, rows), owner * per_brick // rows, 1, 0)
    qm_local = lax.dynamic_slice_in_dim(local[0], owner * per_brick % rows, per_brick, 1)

    at = jnp.stack([grp, dev, jnp.int32(groups), jnp.int32(members)]).astype(jnp.int32)
    alpha_rows = polar.reshape(blocks, width)
    total = fixed.reshape(3 * blocks, width)
    picks = None
    for repeat in range(SWEEPS):
        first, last = repeat == 0, repeat == SWEEPS - 1
        result = sweep(
            at,
            links,
            nearby_targets,
            nearby_polar,
            field,
            coords,
            around,
            weights,
            alpha_rows,
            total,
            first,
            last,
            3 * blocks if first else 0,
        )
        current = result[0]
        if first:
            total = result[1]
        if last:
            picks = result[1]
        else:
            around = exchange(current)
    spread = jnp.broadcast_to(picks[None], (devices,) + picks.shape)
    dipoles = lax.all_to_all(spread, BOTH, 0, 0).reshape(devices * per_brick, width)
    offsets = sorted(chunks)
    sources = jnp.stack([source_of(o) for o in offsets])
    fock_polar = fock_term(sources, [chunks[o] for o in offsets], right_factor, directions, dipoles)
    return (current.reshape(3, 1, 1, sites), qm_local, fock_polar)


def solution(mesh):
    placed = (
        P("grp", "dev"),
        P("dev", "grp"),
        P(None, "dev"),
        P(None, "dev"),
        P(None, "grp", "dev", None),
        P("grp", "dev", None),
        P(None, "grp", "dev", None),
        P("grp", "dev", None, None),
        P("grp", "dev", None),
    )
    return jax.shard_map(
        on_device,
        mesh=mesh,
        in_specs=placed,
        out_specs=(P(None, "grp", "dev", None), P(None, ("grp", "dev")), P("grp", "dev")),
        check_vma=False,
    )
```

```python
import functools

import jax
import jax.numpy as jnp
from jax import lax
from jax.experimental import pallas as pl
from jax.experimental.pallas import tpu as pltpu
from jax.sharding import PartitionSpec as P


SWEEPS = 4
COUPLING = 2e-07
SOFTEN = 4e-05
BRICK = 0.1
SLAB = 0.03
REACH = 2
BOTH = ("grp", "dev")
F32 = jnp.float32
BF16 = jnp.bfloat16
TERMS = 16
PARTS = 2
VMEM = pl.BlockSpec(memory_space=pltpu.VMEM)
SMEM = pl.BlockSpec(memory_space=pltpu.SMEM)


def shift(block, axis, step):
    count = lax.axis_size(axis)
    pairs = [(i, i + step) for i in range(count) if 0 <= i + step < count]
    return lax.ppermute(block, axis, pairs)


def exchange(block):
    low, high = shift(block, "dev", 1), shift(block, "dev", -1)
    column = jnp.stack([low, block, high])
    low, high = shift(column, "grp", 1), shift(column, "grp", -1)
    return low, column, high


def limits(mib):
    return pltpu.CompilerParams(vmem_limit_bytes=mib << 20)


def whole(array):
    return pl.BlockSpec(array.shape, lambda *_: (0,) * len(array.shape))


def ring_order(count):
    return list(range(0, count, 2)) + [i for i in range(count - 1, 0, -1) if i % 2]


def source_of(at_ref, offset, count):
    dev = at_ref[1]
    half = lax.div(dev, 2)
    place = jnp.where(lax.rem(dev, 2) == 0, half, count - 1 - half)
    place = lax.rem(place + offset + count, count)
    return jnp.where(place < (count + 1) // 2, 2 * place, 2 * (count - 1 - place) + 1)


def split(value):
    high = value.astype(BF16).astype(F32)
    rest = value - high
    middle = rest.astype(BF16).astype(F32)
    return high, middle, rest - middle


def weights_kernel(
    per_step, blocks, at_ref, links_ref, low_ref, mid_ref, high_ref, out_ref, coords_ref, far_ref, own_ref, side_ref
):
    width = out_ref.shape[2]
    listed = out_ref.shape[1] // width
    middle_x = (at_ref[0].astype(F32) + 0.5) * BRICK
    middle_y = (at_ref[1].astype(F32) + 0.5) * BRICK
    level = lax.broadcasted_iota(jnp.int32, (blocks, width), 0).astype(F32)
    middle_z = (level + 0.5) * SLAB

    def pieces(x, y, z, more):
        coords = [split(value) for value in (x, y, z)]
        norm = split(x * x + y * y + z * z + more)
        return [c[part] for part in range(3) for c in coords] + list(norm)

    for a, ref in enumerate((low_ref, mid_ref, high_ref)):

        def fill(b, carry, a=a, ref=ref):
            rows = pl.ds(pl.multiple_of((3 * a + b) * blocks, blocks), blocks)
            x = ref[b, :blocks, :] - middle_x
            y = ref[b, blocks : 2 * blocks, :] - middle_y
            z = ref[b, 2 * blocks : 3 * blocks, :] - middle_z
            for k, value in enumerate((x, y, z)):
                coords_ref[k, rows, :] = value
            for at, value in enumerate(pieces(x, y, z, 0.0)):
                far_ref[rows, at, :] = value
            return carry

        lax.fori_loop(0, 3, fill, 0)
    base = slice(4 * blocks, 5 * blocks)
    x, y, middle = coords_ref[0, base, :], coords_ref[1, base, :], coords_ref[2, base, :]

    def own(hop, carry):
        z = middle - (hop - REACH).astype(F32) * SLAB
        for at, value in enumerate(pieces(x, y, z, SOFTEN)):
            own_ref[hop, :, at, :] = value
        return carry

    lax.fori_loop(0, 2 * REACH + 1, own, 0)
    diagonal = lax.broadcasted_iota(jnp.int32, (width, width), 0) == lax.broadcasted_iota(
        jnp.int32, (width, width), 1
    )
    row = lax.broadcasted_iota(jnp.int32, (8, width), 0)
    ones = jnp.ones((3, width), F32)

    def some(step, carry):
        for inner in range(per_step):
            block = step * per_step + inner
            for hop in range(2 * REACH + 1):
                high = -2.0 * own_ref[hop, block, 0:3, :]
                mid = -2.0 * own_ref[hop, block, 3:6, :]
                low = -2.0 * own_ref[hop, block, 6:9, :]
                norm = own_ref[hop, block, 9:12, :]
                none = jnp.zeros((3, width), F32)
                side = jnp.concatenate(
                    [high, high, high, ones, norm, none[:1], mid, mid, none[:2], low, none, none[:2]], axis=0
                )
                side_ref[inner, hop] = side.astype(BF16)
        for inner in range(per_step):
            block = step * per_step + inner
            for n in range(listed):
                link = links_ref[block, n]
                hop = lax.rem(link, blocks) - block + REACH
                top = far_ref[link, 0:8, :]
                end = far_ref[link, 8:16, :]
                end = jnp.where(row < 4, end, jnp.where(row < 7, 1.0, 0.0))
                square = lax.dot_general(
                    jnp.concatenate([top, end, top, top], axis=0).astype(BF16),
                    side_ref[inner, hop],
                    (((0,), (0,)), ((), ())),
                    preferred_element_type=F32,
                )
                root = lax.rsqrt(square)
                two = root * root
                value = two * two * root
                if n == 0:
                    value = jnp.where(diagonal, 0.0, value)
                out_ref[block, n * width : (n + 1) * width, :] = value.astype(BF16)
        return carry

    lax.fori_loop(0, blocks // per_step, some, 0)


def pair_weights(at, links, around, blocks):
    listed = links.shape[1]
    width = around[0].shape[2]
    region = 9 * blocks
    coords = jax.ShapeDtypeStruct((3, region, width), F32)
    return pl.pallas_call(
        functools.partial(weights_kernel, 4, blocks),
        out_shape=[jax.ShapeDtypeStruct((blocks, listed * width, width), BF16), coords],
        in_specs=[SMEM, SMEM] + [VMEM] * 3,
        out_specs=[VMEM, VMEM],
        scratch_shapes=[
            pltpu.VMEM((region, 24, width), F32),
            pltpu.VMEM((2 * REACH + 1, blocks, 24, width), F32),
            pltpu.VMEM((4, 2 * REACH + 1, 32, width), BF16),
        ],
        compiler_params=limits(12),
        name="pair_weights",
    )(at, links, *around)


def sweep_kernel(per_step, blocks, first, last, base, at_ref, links_ref, *refs):
    refs = list(refs)
    if first:
        spot_ref, polar_ref, parts_ref = refs.pop(0), refs.pop(0), refs.pop(0)
    if last:
        target_ref = refs.pop(0)
    coords_ref, low_ref, mid_ref, high_ref, weights_ref, alpha_ref, total_ref, out_ref = refs[:8]
    refs = refs[8:]
    if first:
        sum_ref, field_ref = refs.pop(0), refs.pop(0)
    if last:
        pick_ref = refs.pop(0)
    v_ref, w_ref, p_ref = refs[:3]
    _, width = coords_ref.shape[1:]
    listed = weights_ref.shape[1] // width
    own_base = 4 * blocks
    lane = lax.broadcasted_iota(jnp.int32, (1, width), 1)

    if first:
        scalar_ref, sem = refs[3:]
        parts = parts_ref.shape[0]
        field = parts_ref[0]
        for i in range(1, parts):
            field = field + parts_ref[i]
        field_ref[...] = field
        copy = pltpu.make_async_copy(field_ref, scalar_ref, sem)
        copy.start()
    for a, ref in enumerate((low_ref, mid_ref, high_ref)):
        for b in range(3):
            for k in range(3):
                v_ref[k, (3 * a + b) * blocks : (3 * a + b + 1) * blocks, :] = ref[
                    b, base + k * blocks : base + (k + 1) * blocks, :
                ]
    if first:
        sum_ref[...] = total_ref[...]
        copy.wait()
        groups, members, per_brick = at_ref[2], at_ref[3], at_ref[4]
        lines = field_ref.shape[0] // 3

        def place(p, grp, dev, own):
            t = (grp * members + dev) * per_brick
            line, start = t // width, t % width

            def one(j, carry):
                here = lane == spot_ref[1, p, j]
                row = spot_ref[0, p, j]
                for k in range(3):
                    value = scalar_ref[k * lines + line, start + j]
                    if own:
                        sum_ref[pl.ds(k * blocks + row, 1), :] += jnp.where(here, value, 0.0)
                    else:
                        add = jnp.where(here, value * polar_ref[p, j], 0.0)
                        v_ref[k, pl.ds(p * blocks + row, 1), :] += add
                return carry

            lax.fori_loop(0, spot_ref.shape[2], one, 0, unroll=8)

        def brick(p, carry):
            grp = jnp.clip(at_ref[0] + p // 3 - 1, 0, groups - 1)
            dev = jnp.clip(at_ref[1] + p % 3 - 1, 0, members - 1)
            place(p, grp, dev, False)
            return carry

        lax.fori_loop(0, 9, brick, 0)
        place(4, at_ref[0], at_ref[1], True)

    row = lax.broadcasted_iota(jnp.int32, (TERMS, width), 0)
    which = lax.rem(row, 3)

    def some(step, carry):
        for inner in range(per_step):
            block = step * per_step + inner
            for n in range(listed):
                link = links_ref[block, n]
                away = (lax.rem(link, blocks) - block).astype(F32) * SLAB
                x = coords_ref[0, pl.ds(link, 1), :]
                y = coords_ref[1, pl.ds(link, 1), :]
                z = coords_ref[2, pl.ds(link, 1), :] + away
                v0, v1, v2 = (v_ref[k, pl.ds(link, 1), :] for k in range(3))
                along = x * v0 + y * v1 + z * v2
                third = (x * x + y * y + z * z) * (1.0 / 3.0)
                dipole = jnp.where(which == 0, v0, jnp.where(which == 1, v1, v2))
                spot = jnp.where(
                    row < 3,
                    1.0,
                    jnp.where(
                        (row < 6) | (row == 12), x, jnp.where((row < 9) | (row == 13), y, z)
                    ),
                )
                value = jnp.where(row < 12, spot * dipole, spot * along - third * dipole)
                cols = slice(n * width, (n + 1) * width)
                for part in range(PARTS):
                    piece = value.astype(BF16)
                    w_ref[inner, part * TERMS : (part + 1) * TERMS, cols] = piece
                    if part < PARTS - 1:
                        value = value - piece.astype(F32)
            product = jnp.dot(w_ref[inner], weights_ref[block], preferred_element_type=F32)
            total = product[:TERMS]
            for part in range(1, PARTS):
                total = total + product[part * TERMS : (part + 1) * TERMS]
            p_ref[block] = total
        return carry

    lax.fori_loop(0, blocks // per_step, some, 0)
    x = [coords_ref[k, own_base : own_base + blocks, :] for k in range(3)]
    term = [p_ref[:, r, :] for r in range(15)]
    p = term[:3]
    m = [term[3 + 3 * k : 6 + 3 * k] for k in range(3)]
    q = term[12:15]
    inside = x[0] * p[0] + x[1] * p[1] + x[2] * p[2] - (m[0][0] + m[1][1] + m[2][2])
    size = x[0] * x[0] + x[1] * x[1] + x[2] * x[2] + SOFTEN
    alpha = alpha_ref[...]
    for k in range(3):
        one = x[0] * m[k][0] + x[1] * m[k][1] + x[2] * m[k][2]
        other = x[0] * m[0][k] + x[1] * m[1][k] + x[2] * m[2][k]
        force = x[k] * inside - one + q[k] - (size * p[k] - 2.0 * other) * (1.0 / 3.0)
        rows = slice(k * blocks, (k + 1) * blocks)
        given = sum_ref[rows, :] if first else total_ref[rows, :]
        out_ref[rows, :] = alpha * (given + (3.0 * COUPLING) * force)
    if last:
        per_brick = target_ref.shape[0]
        for j in range(per_brick):
            site = target_ref[j]
            here = lane == site % width
            line = jnp.zeros((1, width), F32)
            for k in range(3):
                values = out_ref[pl.ds(k * blocks + site // width, 1), :]
                found = jnp.sum(jnp.where(here, values, 0.0), axis=1, keepdims=True)
                line = jnp.where(lane == k, found, line)
            pick_ref[0, j : j + 1, :] = line
        for i in range(1, pick_ref.shape[0]):
            pick_ref[i] = pick_ref[0]


def sweep(at, links, coords, around, weights, alpha, total, tail=None, parts=None, target=None, copies=1):
    blocks, depth, width = weights.shape
    region = coords.shape[1]
    first, last = parts is not None, target is not None
    per_step = 8
    rows = jax.ShapeDtypeStruct((3 * blocks, width), F32)
    outs = [rows]
    scratch = [
        pltpu.VMEM((3, region, width), F32),
        pltpu.VMEM((per_step, PARTS * TERMS, depth), BF16),
        pltpu.VMEM((blocks, TERMS, width), F32),
    ]
    given, specs = [at, links], [SMEM, SMEM]
    if first:
        outs += [rows, jax.ShapeDtypeStruct(parts.shape[1:], F32)]
        given += [*tail, parts]
        specs += [SMEM, SMEM, VMEM]
        scratch += [pltpu.SMEM(parts.shape[1:], F32), pltpu.SemaphoreType.DMA]
    if last:
        outs.append(jax.ShapeDtypeStruct((copies, target.shape[0], width), F32))
        given.append(target)
        specs.append(SMEM)
    return pl.pallas_call(
        functools.partial(sweep_kernel, per_step, blocks, first, last, 3 * blocks if first else 0),
        out_shape=outs,
        in_specs=specs + [VMEM] * 7,
        out_specs=[VMEM] * len(outs),
        scratch_shapes=scratch,
        compiler_params=limits(8),
        name="sweep",
    )(*given, coords, *around, weights, alpha, total)


def context_kernel(count, offsets, members, more, at_ref, *refs):
    lefts = refs[:count]
    density_ref = refs[count]
    rights = refs[count + 1 : 2 * count + 1]
    refs = refs[2 * count + 1 :]
    before_ref = refs[0] if more else None
    directions_ref, out_ref, flip_ref, left_ref, sums_ref = refs[-5:]
    step = pl.program_id(0)
    rows = lefts[0].shape[0]

    @pl.when(step == 0)
    def _():
        for i, ref in enumerate(lefts):
            left_ref[i * rows : (i + 1) * rows, :] = ref[...]
        sums_ref[...] = jnp.zeros_like(sums_ref)

    cut = flip_ref.shape[0]
    begin = pl.multiple_of(step * cut, cut)
    flip_ref[...] = jnp.transpose(left_ref[:, pl.ds(begin, cut)])
    context = jnp.dot(left_ref[...], density_ref[...], preferred_element_type=F32)
    lanes = context.shape[1]
    for i, ref in enumerate(rights):
        weighted = context[i * rows : (i + 1) * rows] * ref[...].astype(F32)
        for k in range(3):
            term = weighted * directions_ref[k : k + 1, :]
            folded = term[:, :128]
            for at in range(128, lanes, 128):
                folded = folded + term[:, at : at + 128]
            sums_ref[k, i * rows : (i + 1) * rows, :] += folded

    @pl.when(step == pl.num_programs(0) - 1)
    def _():
        lines = members * rows // 128
        per_line = 128 // rows
        slot = lax.broadcasted_iota(jnp.int32, (1, 128), 1) // rows
        if more:
            out_ref[0] = before_ref[0]
        else:
            out_ref[0] = jnp.zeros_like(out_ref[0])
        for k in range(3):
            for pair in range(sums_ref.shape[1] // 128):
                flipped = jnp.transpose(sums_ref[k, pair * 128 : (pair + 1) * 128, :])
                line = jnp.sum(flipped, axis=0, keepdims=True)
                for inside in range(per_line):
                    i = pair * per_line + inside
                    if i >= count:
                        continue
                    source = source_of(at_ref, offsets[i], members)
                    spread = line
                    for turn in range(1, per_line):
                        spread = jnp.where(
                            slot == (inside + turn) % per_line, pltpu.roll(line, turn * rows, 1), spread
                        )
                    row = k * lines + source // per_line
                    old = out_ref[0, pl.ds(row, 1), :]
                    out_ref[0, pl.ds(row, 1), :] = jnp.where(slot == source % per_line, spread, old)
        for i in range(1, out_ref.shape[0]):
            out_ref[i] = out_ref[0]


def context_field(at, offsets, members, chunks, density, right, directions, before, copies):
    count = len(chunks)
    rows, depth = chunks[0].shape
    columns = density.shape[1]
    tile = 256
    padded = -(-count * rows // 128) * 128
    lines = members * rows // 128
    more = before is not None

    def right_block(offset):
        return pl.BlockSpec((rows, tile), lambda j, at_ref: (source_of(at_ref, offset, members), j))

    out = jax.ShapeDtypeStruct((copies, 3 * lines, 128), F32)
    return pl.pallas_call(
        functools.partial(context_kernel, count, offsets, members, more),
        out_shape=[out, jax.ShapeDtypeStruct((depth, count * rows), BF16)],
        grid_spec=pltpu.PrefetchScalarGridSpec(
            num_scalar_prefetch=1,
            grid=(columns // tile,),
            in_specs=[whole(c) for c in chunks]
            + [pl.BlockSpec((depth, tile), lambda j, at_ref: (0, j))]
            + [right_block(o) for o in offsets]
            + ([whole(before)] if more else [])
            + [pl.BlockSpec((3, tile), lambda j, at_ref: (0, j))],
            out_specs=[
                whole(out),
                pl.BlockSpec((depth * tile // columns, count * rows), lambda j, at_ref: (j, 0)),
            ],
            scratch_shapes=[
                pltpu.VMEM((count * rows, depth), BF16),
                pltpu.VMEM((3, padded, 128), F32),
            ],
        ),
        compiler_params=limits(20),
        name="context_field",
    )(at, *chunks, density, *([right] * count), *([before] if more else []), directions)


def fock_kernel(groups, members, at_ref, *refs):
    count = len(groups)
    lefts = refs[:count]
    right_ref, directions_ref, dipoles_ref, out_ref, scaled_ref = refs[count:]
    rows = right_ref.shape[0] // members

    @pl.when(pl.program_id(0) == 0)
    def _():
        lines = [directions_ref[k : k + 1, :] for k in range(3)]
        for i, offset in enumerate(sum(groups, [])):
            start = pl.multiple_of(source_of(at_ref, offset, members) * rows, rows)
            dipoles = dipoles_ref[pl.ds(start, rows), :]
            along = dipoles[:, 0:1] * lines[0]
            for k in (1, 2):
                along = along + dipoles[:, k : k + 1] * lines[k]
            value = right_ref[pl.ds(start, rows), :].astype(F32) * along
            scaled_ref[i * rows : (i + 1) * rows, :] = (-value).astype(BF16)

    left = jnp.concatenate([ref[...] for ref in lefts], axis=1)
    out_ref[...] = jnp.dot(left, scaled_ref[...], preferred_element_type=F32)


def fock_term(at, groups, members, lefts, right, directions, dipoles):
    depth = lefts[0].shape[0]
    targets, columns = right.shape
    tile = 512
    return pl.pallas_call(
        functools.partial(fock_kernel, groups, members),
        out_shape=jax.ShapeDtypeStruct((depth, columns), F32),
        grid_spec=pltpu.PrefetchScalarGridSpec(
            num_scalar_prefetch=1,
            grid=(depth // tile,),
            in_specs=[pl.BlockSpec((tile, a.shape[1]), lambda i, at_ref: (i, 0)) for a in lefts]
            + [whole(right), whole(directions), whole(dipoles)],
            out_specs=pl.BlockSpec((tile, columns), lambda i, at_ref: (i, 0)),
            scratch_shapes=[pltpu.VMEM((targets, columns), BF16)],
        ),
        name="fock_term",
    )(at, *lefts, right, directions, dipoles)


def on_device(
    density, left_factor, right_factor, directions, places, alpha, static_field, neighbours, targets
):
    groups = lax.axis_size("grp")
    members = lax.axis_size("dev")
    grp = lax.axis_index("grp")
    dev = lax.axis_index("dev")
    rows = left_factor.shape[0]
    per_brick = targets.shape[2]
    sites = places.shape[3]
    blocks = neighbours.shape[2]
    width = sites // blocks
    devices = groups * members
    at = jnp.stack([grp, dev, jnp.int32(groups), jnp.int32(members), jnp.int32(per_brick)]).astype(jnp.int32)

    order = ring_order(members)
    forward = [(order[i], order[(i + 1) % members]) for i in range(members)]
    backward = [(b, a) for a, b in forward]
    chunks = {0: left_factor}
    onward = back = left_factor
    arrivals = [0]
    for step in range(1, members // 2 + 1):
        onward = lax.ppermute(onward, "dev", forward)
        chunks[-step] = onward
        arrivals.append(-step)
        if step <= (members - 1) // 2:
            back = lax.ppermute(back, "dev", backward)
            chunks[step] = back
            arrivals.append(step)

    links = neighbours[0, 0]
    polar = alpha[0, 0]
    own_targets = targets[0, 0]
    fixed = static_field[:, 0, 0]
    picked = jnp.sum(
        jnp.where(own_targets[:, None] == jnp.arange(sites, dtype=jnp.int32)[None, :], polar[None, :], 0.0),
        axis=1,
    )
    tail = jnp.pad(jnp.stack([own_targets.astype(F32), picked]), ((0, 6), (0, width - per_brick)))
    packed = jnp.concatenate(
        [
            places[:, 0, 0].reshape(3 * blocks, width),
            (polar[None] * fixed).reshape(3 * blocks, width),
            tail,
        ]
    )
    around = exchange(packed)
    tails = jnp.stack([a[:, 6 * blocks : 6 * blocks + 2, :per_brick] for a in around])
    tails = tails.reshape(9, 2, per_brick)
    sites_of = tails[:, 0].astype(jnp.int32)
    spots = jnp.stack([sites_of // width, sites_of % width])
    weights, coords = pair_weights(at, links, around, blocks)

    parts_of = [arrivals[i : i + 4] for i in range(0, len(arrivals), 4)]
    parts = None
    lefts = []
    for i, offsets in enumerate(parts_of):
        parts, left = context_field(
            at,
            offsets,
            members,
            [chunks[o] for o in offsets],
            density,
            right_factor,
            directions,
            parts,
            devices if i == len(parts_of) - 1 else 1,
        )
        lefts.append(left)
    parts = lax.all_to_all(parts, BOTH, 0, 0)

    alpha_rows = polar.reshape(blocks, width)
    total = fixed.reshape(3 * blocks, width)
    current, total, field = sweep(
        at, links, coords, around, weights, alpha_rows, total, tail=(spots, tails[:, 1]), parts=parts
    )
    for repeat in range(1, SWEEPS):
        around = exchange(current)
        if repeat < SWEEPS - 1:
            current = sweep(at, links, coords, around, weights, alpha_rows, total)[0]
        else:
            current, picks = sweep(
                at, links, coords, around, weights, alpha_rows, total, target=own_targets, copies=devices
            )
    dipoles = lax.all_to_all(picks, BOTH, 0, 0).reshape(devices * per_brick, width)
    fock_polar = fock_term(at, parts_of, members, lefts, right_factor, directions, dipoles)
    owner = grp * members + dev
    qm_local = lax.dynamic_slice_in_dim(field.reshape(3, members * rows), owner * per_brick, per_brick, 1)
    return (current.reshape(3, 1, 1, sites), qm_local, fock_polar)


def solution(mesh):
    placed = (
        P("grp", "dev"),
        P("dev", "grp"),
        P(None, "dev"),
        P(None, "dev"),
        P(None, "grp", "dev", None),
        P("grp", "dev", None),
        P(None, "grp", "dev", None),
        P("grp", "dev", None, None),
        P("grp", "dev", None),
    )
    return jax.shard_map(
        on_device,
        mesh=mesh,
        in_specs=placed,
        out_specs=(P(None, "grp", "dev", None), P(None, ("grp", "dev")), P("grp", "dev")),
        check_vma=False,
    )
```

```python
import functools

import jax
import jax.numpy as jnp
from jax import lax
from jax.experimental import pallas as pl
from jax.experimental.pallas import tpu as pltpu
from jax.sharding import PartitionSpec as P


SWEEPS = 4
COUPLING = 2e-07
SOFTEN = 4e-05
BRICK = 0.1
SLAB = 0.03
REACH = 2
BOTH = ("grp", "dev")
F32 = jnp.float32
BF16 = jnp.bfloat16
TERMS = 16
PARTS = 2
VMEM = pl.BlockSpec(memory_space=pltpu.VMEM)
SMEM = pl.BlockSpec(memory_space=pltpu.SMEM)


def shift(block, axis, step):
    count = lax.axis_size(axis)
    pairs = [(i, i + step) for i in range(count) if 0 <= i + step < count]
    return lax.ppermute(block, axis, pairs)


def exchange(block):
    low, high = shift(block, "dev", 1), shift(block, "dev", -1)
    column = jnp.stack([low, block, high])
    low, high = shift(column, "grp", 1), shift(column, "grp", -1)
    return low, column, high


def limits(mib):
    return pltpu.CompilerParams(vmem_limit_bytes=mib << 20)


def whole(array):
    return pl.BlockSpec(array.shape, lambda *_: (0,) * len(array.shape))


def ring_order(count):
    return list(range(0, count, 2)) + [i for i in range(count - 1, 0, -1) if i % 2]


def source_of(at_ref, offset, count):
    dev = at_ref[1]
    half = lax.div(dev, 2)
    place = jnp.where(lax.rem(dev, 2) == 0, half, count - 1 - half)
    place = lax.rem(place + offset + count, count)
    return jnp.where(place < (count + 1) // 2, 2 * place, 2 * (count - 1 - place) + 1)


def split(value):
    high = value.astype(BF16).astype(F32)
    rest = value - high
    middle = rest.astype(BF16).astype(F32)
    return high, middle, rest - middle


def weights_kernel(
    per_step, blocks, at_ref, links_ref, low_ref, mid_ref, high_ref, out_ref, coords_ref, far_ref, own_ref, side_ref
):
    width = out_ref.shape[2]
    listed = out_ref.shape[1] // width
    middle_x = (at_ref[0].astype(F32) + 0.5) * BRICK
    middle_y = (at_ref[1].astype(F32) + 0.5) * BRICK
    level = lax.broadcasted_iota(jnp.int32, (blocks, width), 0).astype(F32)
    middle_z = (level + 0.5) * SLAB

    def pieces(x, y, z, more):
        coords = [split(value) for value in (x, y, z)]
        norm = split(x * x + y * y + z * z + more)
        return [c[part] for part in range(3) for c in coords] + list(norm)

    for a, ref in enumerate((low_ref, mid_ref, high_ref)):

        def fill(b, carry, a=a, ref=ref):
            rows = pl.ds(pl.multiple_of((3 * a + b) * blocks, blocks), blocks)
            x = ref[b, :blocks, :] - middle_x
            y = ref[b, blocks : 2 * blocks, :] - middle_y
            z = ref[b, 2 * blocks : 3 * blocks, :] - middle_z
            for k, value in enumerate((x, y, z)):
                coords_ref[k, rows, :] = value
            for at, value in enumerate(pieces(x, y, z, 0.0)):
                far_ref[rows, at, :] = value
            return carry

        lax.fori_loop(0, 3, fill, 0)
    base = slice(4 * blocks, 5 * blocks)
    x, y, middle = coords_ref[0, base, :], coords_ref[1, base, :], coords_ref[2, base, :]

    def own(hop, carry):
        z = middle - (hop - REACH).astype(F32) * SLAB
        for at, value in enumerate(pieces(x, y, z, SOFTEN)):
            own_ref[hop, :, at, :] = value
        return carry

    lax.fori_loop(0, 2 * REACH + 1, own, 0)
    diagonal = lax.broadcasted_iota(jnp.int32, (width, width), 0) == lax.broadcasted_iota(
        jnp.int32, (width, width), 1
    )
    row = lax.broadcasted_iota(jnp.int32, (8, width), 0)
    ones = jnp.ones((3, width), F32)

    def some(step, carry):
        for inner in range(per_step):
            block = step * per_step + inner
            for hop in range(2 * REACH + 1):
                high = -2.0 * own_ref[hop, block, 0:3, :]
                mid = -2.0 * own_ref[hop, block, 3:6, :]
                low = -2.0 * own_ref[hop, block, 6:9, :]
                norm = own_ref[hop, block, 9:12, :]
                none = jnp.zeros((3, width), F32)
                side = jnp.concatenate(
                    [high, high, high, ones, norm, none[:1], mid, mid, none[:2], low, none, none[:2]], axis=0
                )
                side_ref[inner, hop] = side.astype(BF16)
        for inner in range(per_step):
            block = step * per_step + inner
            for n in range(listed):
                link = links_ref[block, n]
                hop = lax.rem(link, blocks) - block + REACH
                top = far_ref[link, 0:8, :]
                end = far_ref[link, 8:16, :]
                end = jnp.where(row < 4, end, jnp.where(row < 7, 1.0, 0.0))
                square = lax.dot_general(
                    jnp.concatenate([top, end, top, top], axis=0).astype(BF16),
                    side_ref[inner, hop],
                    (((0,), (0,)), ((), ())),
                    preferred_element_type=F32,
                )
                root = lax.rsqrt(square)
                two = root * root
                value = two * two * root
                if n == 0:
                    value = jnp.where(diagonal, 0.0, value)
                out_ref[block, n * width : (n + 1) * width, :] = value.astype(BF16)
        return carry

    lax.fori_loop(0, blocks // per_step, some, 0)


def pair_weights(at, links, around, blocks):
    listed = links.shape[1]
    width = around[0].shape[2]
    region = 9 * blocks
    coords = jax.ShapeDtypeStruct((3, region, width), F32)
    return pl.pallas_call(
        functools.partial(weights_kernel, 4, blocks),
        out_shape=[jax.ShapeDtypeStruct((blocks, listed * width, width), BF16), coords],
        in_specs=[SMEM, SMEM] + [VMEM] * 3,
        out_specs=[VMEM, VMEM],
        scratch_shapes=[
            pltpu.VMEM((region, 24, width), F32),
            pltpu.VMEM((2 * REACH + 1, blocks, 24, width), F32),
            pltpu.VMEM((4, 2 * REACH + 1, 32, width), BF16),
        ],
        compiler_params=limits(12),
        name="pair_weights",
    )(at, links, *around)


def sweep_kernel(per_step, blocks, first, last, base, at_ref, links_ref, *refs):
    refs = list(refs)
    if first:
        spot_ref, polar_ref, parts_ref = refs.pop(0), refs.pop(0), refs.pop(0)
    else:
        own_ref = refs.pop(0)
    if last:
        target_ref = refs.pop(0)
    coords_ref, low_ref, mid_ref, high_ref, weights_ref, alpha_ref, total_ref, out_ref = refs[:8]
    refs = refs[8:]
    if not last:
        halo_ref = refs.pop(0)
    if first:
        sum_ref, field_ref = refs.pop(0), refs.pop(0)
    if last:
        pick_ref = refs.pop(0)
    v_ref, w_ref, p_ref = refs[:3]
    _, width = coords_ref.shape[1:]
    listed = weights_ref.shape[1] // width
    own_base = 4 * blocks
    lane = lax.broadcasted_iota(jnp.int32, (1, width), 1)

    if first:
        scalar_ref, sem = refs[3:]
        parts = parts_ref.shape[0]
        field = parts_ref[0]
        for i in range(1, parts):
            field = field + parts_ref[i]
        field_ref[...] = field
        copy = pltpu.make_async_copy(field_ref, scalar_ref, sem)
        copy.start()
    for a, ref in enumerate((low_ref, mid_ref, high_ref)):
        for b in range(3):
            for k in range(3):
                rows = slice(base + k * blocks, base + (k + 1) * blocks)
                given = own_ref[rows, :] if (a, b) == (1, 1) and not first else ref[b, rows, :]
                v_ref[k, (3 * a + b) * blocks : (3 * a + b + 1) * blocks, :] = given.astype(F32)
    if first:
        sum_ref[...] = total_ref[...]
        copy.wait()
        groups, members, per_brick = at_ref[2], at_ref[3], at_ref[4]
        lines = field_ref.shape[0] // 3

        def place(p, grp, dev, own):
            t = (grp * members + dev) * per_brick
            line, start = t // width, t % width

            def one(j, carry):
                here = lane == spot_ref[1, p, j]
                row = spot_ref[0, p, j]
                for k in range(3):
                    value = scalar_ref[k * lines + line, start + j]
                    if own:
                        sum_ref[pl.ds(k * blocks + row, 1), :] += jnp.where(here, value, 0.0)
                    else:
                        add = jnp.where(here, value * polar_ref[p, j], 0.0)
                        v_ref[k, pl.ds(p * blocks + row, 1), :] += add
                return carry

            lax.fori_loop(0, spot_ref.shape[2], one, 0, unroll=8)

        def brick(p, carry):
            grp = jnp.clip(at_ref[0] + p // 3 - 1, 0, groups - 1)
            dev = jnp.clip(at_ref[1] + p % 3 - 1, 0, members - 1)
            place(p, grp, dev, False)
            return carry

        lax.fori_loop(0, 9, brick, 0)
        place(4, at_ref[0], at_ref[1], True)

    row = lax.broadcasted_iota(jnp.int32, (TERMS, width), 0)
    which = lax.rem(row, 3)

    def some(step, carry):
        for inner in range(per_step):
            block = step * per_step + inner
            for n in range(listed):
                link = links_ref[block, n]
                away = (lax.rem(link, blocks) - block).astype(F32) * SLAB
                x = coords_ref[0, pl.ds(link, 1), :]
                y = coords_ref[1, pl.ds(link, 1), :]
                z = coords_ref[2, pl.ds(link, 1), :] + away
                v0, v1, v2 = (v_ref[k, pl.ds(link, 1), :] for k in range(3))
                along = x * v0 + y * v1 + z * v2
                third = (x * x + y * y + z * z) * (1.0 / 3.0)
                dipole = jnp.where(which == 0, v0, jnp.where(which == 1, v1, v2))
                spot = jnp.where(
                    row < 3,
                    1.0,
                    jnp.where(
                        (row < 6) | (row == 12), x, jnp.where((row < 9) | (row == 13), y, z)
                    ),
                )
                value = jnp.where(row < 12, spot * dipole, spot * along - third * dipole)
                cols = slice(n * width, (n + 1) * width)
                for part in range(PARTS):
                    piece = value.astype(BF16)
                    w_ref[inner, part * TERMS : (part + 1) * TERMS, cols] = piece
                    if part < PARTS - 1:
                        value = value - piece.astype(F32)
            product = jnp.dot(w_ref[inner], weights_ref[block], preferred_element_type=F32)
            total = product[:TERMS]
            for part in range(1, PARTS):
                total = total + product[part * TERMS : (part + 1) * TERMS]
            p_ref[block] = total
        return carry

    lax.fori_loop(0, blocks // per_step, some, 0)
    x = [coords_ref[k, own_base : own_base + blocks, :] for k in range(3)]
    term = [p_ref[:, r, :] for r in range(15)]
    p = term[:3]
    m = [term[3 + 3 * k : 6 + 3 * k] for k in range(3)]
    q = term[12:15]
    inside = x[0] * p[0] + x[1] * p[1] + x[2] * p[2] - (m[0][0] + m[1][1] + m[2][2])
    size = x[0] * x[0] + x[1] * x[1] + x[2] * x[2] + SOFTEN
    alpha = alpha_ref[...]
    for k in range(3):
        one = x[0] * m[k][0] + x[1] * m[k][1] + x[2] * m[k][2]
        other = x[0] * m[0][k] + x[1] * m[1][k] + x[2] * m[2][k]
        force = x[k] * inside - one + q[k] - (size * p[k] - 2.0 * other) * (1.0 / 3.0)
        rows = slice(k * blocks, (k + 1) * blocks)
        given = sum_ref[rows, :] if first else total_ref[rows, :]
        value = alpha * (given + (3.0 * COUPLING) * force)
        out_ref[rows, :] = value
        if not last:
            halo_ref[rows, :] = value.astype(BF16)
    if last:
        per_brick = target_ref.shape[0]
        for j in range(per_brick):
            site = target_ref[j]
            here = lane == site % width
            line = jnp.zeros((1, width), F32)
            for k in range(3):
                values = out_ref[pl.ds(k * blocks + site // width, 1), :]
                found = jnp.sum(jnp.where(here, values, 0.0), axis=1, keepdims=True)
                line = jnp.where(lane == k, found, line)
            pick_ref[0, j : j + 1, :] = line
        for i in range(1, pick_ref.shape[0]):
            pick_ref[i] = pick_ref[0]


def sweep(at, links, coords, around, weights, alpha, total, tail=None, parts=None, own=None, target=None, copies=1):
    blocks, depth, width = weights.shape
    region = coords.shape[1]
    first, last = parts is not None, target is not None
    per_step = 8
    rows = jax.ShapeDtypeStruct((3 * blocks, width), F32)
    outs = [rows] if last else [rows, jax.ShapeDtypeStruct((3 * blocks, width), BF16)]
    scratch = [
        pltpu.VMEM((3, region, width), F32),
        pltpu.VMEM((per_step, PARTS * TERMS, depth), BF16),
        pltpu.VMEM((blocks, TERMS, width), F32),
    ]
    given, specs = [at, links], [SMEM, SMEM]
    if first:
        outs += [rows, jax.ShapeDtypeStruct(parts.shape[1:], F32)]
        given += [*tail, parts]
        specs += [SMEM, SMEM, VMEM]
        scratch += [pltpu.SMEM(parts.shape[1:], F32), pltpu.SemaphoreType.DMA]
    else:
        given.append(own)
        specs.append(VMEM)
    if last:
        outs.append(jax.ShapeDtypeStruct((copies, target.shape[0], width), F32))
        given.append(target)
        specs.append(SMEM)
    return pl.pallas_call(
        functools.partial(sweep_kernel, per_step, blocks, first, last, 3 * blocks if first else 0),
        out_shape=outs,
        in_specs=specs + [VMEM] * 7,
        out_specs=[VMEM] * len(outs),
        scratch_shapes=scratch,
        compiler_params=limits(8),
        name="sweep",
    )(*given, coords, *around, weights, alpha, total)


def context_kernel(count, offsets, members, more, at_ref, *refs):
    lefts = refs[:count]
    density_ref = refs[count]
    rights = refs[count + 1 : 2 * count + 1]
    refs = refs[2 * count + 1 :]
    before_ref = refs[0] if more else None
    directions_ref, out_ref, flip_ref, left_ref, sums_ref = refs[-5:]
    step = pl.program_id(0)
    rows = lefts[0].shape[0]

    @pl.when(step == 0)
    def _():
        for i, ref in enumerate(lefts):
            left_ref[i * rows : (i + 1) * rows, :] = ref[...]
        sums_ref[...] = jnp.zeros_like(sums_ref)

    cut = flip_ref.shape[0]
    begin = pl.multiple_of(step * cut, cut)
    flip_ref[...] = jnp.transpose(left_ref[:, pl.ds(begin, cut)])
    context = jnp.dot(left_ref[...], density_ref[...], preferred_element_type=F32)
    lanes = context.shape[1]
    for i, ref in enumerate(rights):
        weighted = context[i * rows : (i + 1) * rows] * ref[...].astype(F32)
        for k in range(3):
            term = weighted * directions_ref[k : k + 1, :]
            folded = term[:, :128]
            for at in range(128, lanes, 128):
                folded = folded + term[:, at : at + 128]
            sums_ref[k, i * rows : (i + 1) * rows, :] += folded

    @pl.when(step == pl.num_programs(0) - 1)
    def _():
        lines = members * rows // 128
        per_line = 128 // rows
        slot = lax.broadcasted_iota(jnp.int32, (1, 128), 1) // rows
        if more:
            out_ref[0] = before_ref[0]
        else:
            out_ref[0] = jnp.zeros_like(out_ref[0])
        for k in range(3):
            for pair in range(sums_ref.shape[1] // 128):
                flipped = jnp.transpose(sums_ref[k, pair * 128 : (pair + 1) * 128, :])
                line = jnp.sum(flipped, axis=0, keepdims=True)
                for inside in range(per_line):
                    i = pair * per_line + inside
                    if i >= count:
                        continue
                    source = source_of(at_ref, offsets[i], members)
                    spread = line
                    for turn in range(1, per_line):
                        spread = jnp.where(
                            slot == (inside + turn) % per_line, pltpu.roll(line, turn * rows, 1), spread
                        )
                    row = k * lines + source // per_line
                    old = out_ref[0, pl.ds(row, 1), :]
                    out_ref[0, pl.ds(row, 1), :] = jnp.where(slot == source % per_line, spread, old)
        for i in range(1, out_ref.shape[0]):
            out_ref[i] = out_ref[0]


def context_field(at, offsets, members, chunks, density, right, directions, before, copies):
    count = len(chunks)
    rows, depth = chunks[0].shape
    columns = density.shape[1]
    tile = 256
    padded = -(-count * rows // 128) * 128
    lines = members * rows // 128
    more = before is not None

    def right_block(offset):
        return pl.BlockSpec((rows, tile), lambda j, at_ref: (source_of(at_ref, offset, members), j))

    out = jax.ShapeDtypeStruct((copies, 3 * lines, 128), F32)
    return pl.pallas_call(
        functools.partial(context_kernel, count, offsets, members, more),
        out_shape=[out, jax.ShapeDtypeStruct((depth, count * rows), BF16)],
        grid_spec=pltpu.PrefetchScalarGridSpec(
            num_scalar_prefetch=1,
            grid=(columns // tile,),
            in_specs=[whole(c) for c in chunks]
            + [pl.BlockSpec((depth, tile), lambda j, at_ref: (0, j))]
            + [right_block(o) for o in offsets]
            + ([whole(before)] if more else [])
            + [pl.BlockSpec((3, tile), lambda j, at_ref: (0, j))],
            out_specs=[
                whole(out),
                pl.BlockSpec((depth * tile // columns, count * rows), lambda j, at_ref: (j, 0)),
            ],
            scratch_shapes=[
                pltpu.VMEM((count * rows, depth), BF16),
                pltpu.VMEM((3, padded, 128), F32),
            ],
        ),
        compiler_params=limits(20),
        name="context_field",
    )(at, *chunks, density, *([right] * count), *([before] if more else []), directions)


def fock_kernel(groups, members, at_ref, *refs):
    count = len(groups)
    lefts = refs[:count]
    right_ref, directions_ref, dipoles_ref, out_ref, scaled_ref = refs[count:]
    rows = right_ref.shape[0] // members

    @pl.when(pl.program_id(0) == 0)
    def _():
        lines = [directions_ref[k : k + 1, :] for k in range(3)]
        for i, offset in enumerate(sum(groups, [])):
            start = pl.multiple_of(source_of(at_ref, offset, members) * rows, rows)
            dipoles = dipoles_ref[pl.ds(start, rows), :]
            along = dipoles[:, 0:1] * lines[0]
            for k in (1, 2):
                along = along + dipoles[:, k : k + 1] * lines[k]
            value = right_ref[pl.ds(start, rows), :].astype(F32) * along
            scaled_ref[i * rows : (i + 1) * rows, :] = (-value).astype(BF16)

    left = jnp.concatenate([ref[...] for ref in lefts], axis=1)
    out_ref[...] = jnp.dot(left, scaled_ref[...], preferred_element_type=F32)


def fock_term(at, groups, members, lefts, right, directions, dipoles):
    depth = lefts[0].shape[0]
    targets, columns = right.shape
    tile = 512
    return pl.pallas_call(
        functools.partial(fock_kernel, groups, members),
        out_shape=jax.ShapeDtypeStruct((depth, columns), F32),
        grid_spec=pltpu.PrefetchScalarGridSpec(
            num_scalar_prefetch=1,
            grid=(depth // tile,),
            in_specs=[pl.BlockSpec((tile, a.shape[1]), lambda i, at_ref: (i, 0)) for a in lefts]
            + [whole(right), whole(directions), whole(dipoles)],
            out_specs=pl.BlockSpec((tile, columns), lambda i, at_ref: (i, 0)),
            scratch_shapes=[pltpu.VMEM((targets, columns), BF16)],
        ),
        name="fock_term",
    )(at, *lefts, right, directions, dipoles)


def on_device(
    density, left_factor, right_factor, directions, places, alpha, static_field, neighbours, targets
):
    groups = lax.axis_size("grp")
    members = lax.axis_size("dev")
    grp = lax.axis_index("grp")
    dev = lax.axis_index("dev")
    rows = left_factor.shape[0]
    per_brick = targets.shape[2]
    sites = places.shape[3]
    blocks = neighbours.shape[2]
    width = sites // blocks
    devices = groups * members
    at = jnp.stack([grp, dev, jnp.int32(groups), jnp.int32(members), jnp.int32(per_brick)]).astype(jnp.int32)

    order = ring_order(members)
    forward = [(order[i], order[(i + 1) % members]) for i in range(members)]
    backward = [(b, a) for a, b in forward]
    chunks = {0: left_factor}
    onward = back = left_factor
    arrivals = [0]
    for step in range(1, members // 2 + 1):
        onward = lax.ppermute(onward, "dev", forward)
        chunks[-step] = onward
        arrivals.append(-step)
        if step <= (members - 1) // 2:
            back = lax.ppermute(back, "dev", backward)
            chunks[step] = back
            arrivals.append(step)

    links = neighbours[0, 0]
    polar = alpha[0, 0]
    own_targets = targets[0, 0]
    fixed = static_field[:, 0, 0]
    picked = jnp.sum(
        jnp.where(own_targets[:, None] == jnp.arange(sites, dtype=jnp.int32)[None, :], polar[None, :], 0.0),
        axis=1,
    )
    tail = jnp.pad(jnp.stack([own_targets.astype(F32), picked]), ((0, 6), (0, width - per_brick)))
    packed = jnp.concatenate(
        [
            places[:, 0, 0].reshape(3 * blocks, width),
            (polar[None] * fixed).reshape(3 * blocks, width),
            tail,
        ]
    )
    around = exchange(packed)
    tails = jnp.stack([a[:, 6 * blocks : 6 * blocks + 2, :per_brick] for a in around])
    tails = tails.reshape(9, 2, per_brick)
    sites_of = tails[:, 0].astype(jnp.int32)
    spots = jnp.stack([sites_of // width, sites_of % width])
    weights, coords = pair_weights(at, links, around, blocks)

    parts_of = [arrivals[i : i + 4] for i in range(0, len(arrivals), 4)]
    parts = None
    lefts = []
    for i, offsets in enumerate(parts_of):
        parts, left = context_field(
            at,
            offsets,
            members,
            [chunks[o] for o in offsets],
            density,
            right_factor,
            directions,
            parts,
            devices if i == len(parts_of) - 1 else 1,
        )
        lefts.append(left)
    parts = lax.all_to_all(parts, BOTH, 0, 0)

    alpha_rows = polar.reshape(blocks, width)
    total = fixed.reshape(3 * blocks, width)
    current, halo, total, field = sweep(
        at, links, coords, around, weights, alpha_rows, total, tail=(spots, tails[:, 1]), parts=parts
    )
    for repeat in range(1, SWEEPS):
        around = exchange(halo)
        if repeat < SWEEPS - 1:
            current, halo = sweep(at, links, coords, around, weights, alpha_rows, total, own=current)
        else:
            current, picks = sweep(
                at,
                links,
                coords,
                around,
                weights,
                alpha_rows,
                total,
                own=current,
                target=own_targets,
                copies=devices,
            )
    dipoles = lax.all_to_all(picks, BOTH, 0, 0).reshape(devices * per_brick, width)
    fock_polar = fock_term(at, parts_of, members, lefts, right_factor, directions, dipoles)
    owner = grp * members + dev
    qm_local = lax.dynamic_slice_in_dim(field.reshape(3, members * rows), owner * per_brick, per_brick, 1)
    return (current.reshape(3, 1, 1, sites), qm_local, fock_polar)


def solution(mesh):
    placed = (
        P("grp", "dev"),
        P("dev", "grp"),
        P(None, "dev"),
        P(None, "dev"),
        P(None, "grp", "dev", None),
        P("grp", "dev", None),
        P(None, "grp", "dev", None),
        P("grp", "dev", None, None),
        P("grp", "dev", None),
    )
    return jax.shard_map(
        on_device,
        mesh=mesh,
        in_specs=placed,
        out_specs=(P(None, "grp", "dev", None), P(None, ("grp", "dev")), P("grp", "dev")),
        check_vma=False,
    )
```
